256 devices in a mesh: vocab: 64 (over y, z, core), batch: 4 (over x).
Axes of the slice: x: 4, y: 4, z: 8, core: 2. Of those that a mesh axis runs over, the one named last changes fastest.
Arguments:
- latent_vectors: bfloat16 [2048, 4608], P(('batch', 'vocab')), parts along dimension 0, may hold values from -8 to 8
- unembedding_matrix: bfloat16 [18432, 65536], P('batch', 'vocab'), parts along dimension 0, may hold values from -1 to 1
- sampler_heat: float32 [2048], P('batch'), parts along dimension 0, may hold values from 0.1 to 1
Outputs:
- probs: bfloat16 [2048, 65536], P(('batch', 'vocab')), parts along dimension 0
- lse: float32 [2048], P(('batch', 'vocab')), parts along dimension 0
- z_loss: float32 [2048], P(('batch', 'vocab')), parts along dimension 0
The draws below stay inside these ranges and needn't reach their ends.
There are 4 independent parts, one for each index of `batch`. The reference program is written for one: setup_inputs(seed, part) draws one part's arguments, and reference() takes and returns one part's arrays. A program takes and returns all parts, laid end to end along the dimension named above; each array names one. Nothing has to cross between parts.
All inputs are finite; a program needn't handle non-finite values.
Results may differ from the reference program's by a relative error of at most 0.00115.
Values may be sent and summed in bfloat16 or wider, within the bound.
No kernel may reach another device: no remote copies, remote signals or barrier semaphores. Data moves between devices by JAX's collectives and lax.ppermute only.
A program may use at most 64 MiB of HBM per device.

```python
import math
import jax
import jax.numpy as jnp

D = 4608
PROMPT_NUMBER = 512
VOCAB = 65536


def vocab_weight(key):
    gaussian_draw = jax.random.normal(jax.random.fold_in(key, 11), (D, VOCAB), jnp.float32)
    return jnp.clip(gaussian_draw, -4.0, 4.0) / math.sqrt(D)


def draw_unembedding_matrix(key, part):
    return vocab_weight(key).astype(jnp.bfloat16)


def draw_latent_vectors(key, part):
    hidden_states = jnp.clip(jax.random.normal(jax.random.fold_in(key, 23), (PROMPT_NUMBER, D), jnp.float32), -6.0, 6.0)
    return hidden_states.astype(jnp.bfloat16)


def draw_sampler_heat(key, part):
    heat = jax.random.uniform(jax.random.fold_in(key, 41), (PROMPT_NUMBER,), jnp.float32, 0.8, 1.0)
    return heat.astype(jnp.float32)


def setup_inputs(seed: int = 0, part: int = 0) -> dict:
    splits = jax.random.split(jax.random.key(seed), 4)
    part_splits = jax.random.split(jax.random.fold_in(splits[3], part), 4)
    return {
        "latent_vectors": draw_latent_vectors(jax.random.fold_in(jax.random.fold_in(splits[3], part), 71), part),
        "unembedding_matrix": draw_unembedding_matrix(jax.random.fold_in(jax.random.fold_in(splits[3], part), 71), part),
        "sampler_heat": draw_sampler_heat(jax.random.fold_in(jax.random.fold_in(splits[3], part), 71), part),
    }


def reference(latent_vectors, unembedding_matrix, sampler_heat):
    logits = jnp.dot(latent_vectors, unembedding_matrix, preferred_element_type=jnp.float32)
    bounded_scores = 30.0 * jnp.tanh(logits / 30.0)
    heat_scaled_scores = bounded_scores / sampler_heat[:, None]
    peak = jnp.max(heat_scaled_scores, axis=1)
    total = jnp.sum(jnp.exp(heat_scaled_scores - peak[:, None]), axis=1)
    lse = peak + jnp.log(total)
    z_loss = 0.0001 * lse * lse
    probs = jnp.exp(heat_scaled_scores - lse[:, None]).astype(jnp.bfloat16)
    return probs, lse, z_loss
```

```python
import jax
import jax.numpy as jnp
from jax import lax
from jax.sharding import Mesh, PartitionSpec as P


NY, NZ = 4, 8
V = ("y", "z", "core")


def _index(y, z, c):
    return ((y % NY) * NZ + z % NZ) * 2 + c


def _pairs(dy, dz, dc):
    out = []
    for y in range(NY):
        for z in range(NZ):
            for c in range(2):
                way = 1 - 2 * c
                out.append((_index(y, z, c), _index(y + way * dy, z + way * dz, c ^ dc)))
    return out


def along_y(value):
    return lax.ppermute(value, V, _pairs(1, 0, 0))


def along_z(value):
    return lax.ppermute(value, V, _pairs(0, 1, 0))


def swapped(value):
    return lax.ppermute(value, V, _pairs(0, 0, 1))


def put(whole, piece, *at):
    lead = len(at)
    shape, start = list(whole.shape), []
    for k in range(whole.ndim):
        if k < lead and at[k] is not None:
            shape[k] = 1
            start.append(at[k])
        else:
            start.append(0)
    return lax.dynamic_update_slice(whole, piece.reshape(shape), start)


def ring(unit, move, me, size, core, axis):
    half = size // 2
    toward = 2 * core - 1
    blocks, held = [(me, unit, None)], unit
    for step in range(1, half):
        held = move(held)
        blocks.append(((me + size + toward * step) % size, held, None))
        blocks.append(((me + size - toward * step) % size, swapped(held), None))
    part = move(lax.dynamic_index_in_dim(held, core, axis, keepdims=False))
    blocks.append(((me + half) % size, part, core))
    blocks.append(((me + half) % size, swapped(part), 1 - core))
    return blocks


def gathered(x):
    y, z, core = (lax.axis_index(name) for name in V)
    rows, depth = x.shape
    pair = put(put(jnp.zeros((2, rows, depth), x.dtype), x, core), swapped(x), 1 - core)
    cut = depth // 2
    whole = jnp.zeros((NZ, NY, 2, rows, depth), x.dtype)

    near = pair[:, :, :cut]
    far = pair[:, :, cut:]
    column = jnp.zeros((NY, 2, rows, cut), x.dtype)
    line = jnp.zeros((NZ, 2, rows, depth - cut), x.dtype)
    for at, block, half in ring(near, along_y, y, NY, core, 0):
        column = put(column, block, at) if half is None else put(column, block, at, half)
    for at, block, half in ring(far, along_z, z, NZ, core, 0):
        line = put(line, block, at) if half is None else put(line, block, at, half)
    pieces = []
    for at, block, half in ring(column, along_z, z, NZ, core, 1):
        spot = (at, 0, 0, 0, 0) if half is None else (at, 0, half, 0, 0)
        shape = (1, NY, 2, rows, cut) if half is None else (1, NY, 1, rows, cut)
        pieces.append((block.reshape(shape), spot))
    for at, block, half in ring(line, along_y, y, NY, core, 1):
        spot = (0, at, 0, 0, cut) if half is None else (0, at, half, 0, cut)
        shape = (NZ, 1, 2, rows, depth - cut) if half is None else (NZ, 1, 1, rows, depth - cut)
        pieces.append((block.reshape(shape), spot))
    for block, spot in pieces:
        whole = lax.dynamic_update_slice(whole, block, spot)
    return whole.reshape(-1, depth)


def local(latent_vectors, unembedding_matrix, sampler_heat):
    seq_own = latent_vectors.shape[0]
    y, z, core = (lax.axis_index(name) for name in V)
    heat = sampler_heat.reshape(NY, NZ, -1).transpose(1, 0, 2).reshape(-1, 1)
    logits = jnp.dot(
        gathered(latent_vectors), unembedding_matrix, preferred_element_type=jnp.float32
    )
    scaled = 30.0 * jnp.tanh(logits / 30.0) / heat
    peak = jnp.max(scaled, axis=1)
    total = jnp.sum(jnp.exp(scaled - peak[:, None]), axis=1)
    part = peak + jnp.log(total)
    parts = lax.all_to_all(
        jnp.broadcast_to(part, (2 * NY * NZ, part.size)), V, 0, 0, tiled=True
    )
    top = jnp.max(parts, axis=0)
    lse = top + jnp.log(jnp.sum(jnp.exp(parts - top), axis=0))
    tiles = jnp.exp(scaled - lse[:, None]).astype(jnp.bfloat16)
    tiles = tiles.reshape(NZ, NY, 2 * seq_own, -1).transpose(1, 0, 2, 3).reshape(tiles.shape)
    probs = lax.all_to_all(tiles, V, split_axis=0, concat_axis=1, tiled=True)
    own = lax.dynamic_slice_in_dim(lse, ((z * NY + y) * 2 + core) * seq_own, seq_own, 0)
    return probs, own, 0.0001 * own * own


def solution(mesh):
    parts = Mesh(mesh.devices.reshape(NY, NZ, 2, -1), (*V, "batch"))
    rows = ("batch", *V)
    in_specs = (P(rows, None), P("batch", V), P("batch"))
    out_specs = (P(rows, None), P(rows), P(rows))
    return jax.shard_map(local, mesh=parts, in_specs=in_specs, out_specs=out_specs, check_vma=False)
```
